32 devices in a mesh: gx: 4 (over y, x), gy: 2 (over core), gz: 4 (over z).
Axes of the slice: x: 2, y: 2, z: 4, core: 2. Of those that a mesh axis runs over, the one named last changes fastest.
Arguments:
- positions: float32 [3, 8, 8, 8, 128], P(None, 'gx', 'gy', 'gz'), may hold values from 0 to 1
- type_ids: int32 [8, 8, 8, 128], P('gx', 'gy', 'gz'), may hold values from 0 to 1
- counts: int32 [8, 8, 8], P('gx', 'gy', 'gz'), may hold values from 64 to 128
- type_charge: float32 [2], replicated, may hold values from -1 to 1
- type_sigma: float32 [2], replicated, may hold values from 0.2 to 0.35
- type_epsilon: float32 [2], replicated, may hold values from 0.05 to 0.5
Outputs:
- forces: float32 [3, 8, 8, 8, 128], P(None, 'gx', 'gy', 'gz')
- totals: float32 [2], replicated
The draws below stay inside these ranges and needn't reach their ends.
All inputs are finite; a program needn't handle non-finite values.
Results may differ from the reference program's by a relative error of at most 0.0003.
Values sent between devices are 32-bit elements; how exact they have to be, the bound alone decides.
A program may use at most 64 MiB of HBM per device.

```python
import math
import jax
import jax.numpy as jnp
from jax import lax

ATOMS_CELL = 128
TYPES = 2
NX = 8
NY = 8
NZ = 8


def plant(result, stream_key, smallest, top_value):
    dims = result.shape
    spot = [jax.random.randint(jax.random.fold_in(stream_key, axis), (), 0, dims[axis]) for axis in range(len(dims))]
    result = result.at[tuple(spot)].set(smallest)
    longest = dims.index(max(dims))
    spot[longest] = (spot[longest] + 1) % dims[longest]
    return result.at[tuple(spot)].set(top_value)


def block_scale(own_key, shape, split, low, high):
    factor_of = 1.0
    for axis_at, shards_of in split:
        steps = jax.random.uniform(jax.random.fold_in(jax.random.fold_in(own_key, 6), axis_at), (shards_of,), jnp.float32, low / len(split), high / len(split))
        factor_of = factor_of * jnp.repeat(jnp.exp(steps), shape[axis_at] // shards_of).reshape((-1,) + (1,) * (len(shape) - 1 - axis_at))
    return factor_of


def setup_inputs(seed: int = 0) -> dict:
    key_of = jax.random.split(jax.random.key(seed), 7)
    return {
        "positions": jnp.clip(1.0 * jax.random.uniform(key_of[0], (3, NX, NY, NZ, ATOMS_CELL), jnp.float32) ** block_scale(key_of[0], (3, NX, NY, NZ, ATOMS_CELL), ((1, 4), (2, 2), (3, 4)), -0.2, 0.2), 0.0, 1.0),
        "type_ids": plant(jax.random.randint(key_of[1], (NX, NY, NZ, ATOMS_CELL), 0, TYPES), jax.random.fold_in(key_of[1], 1), 0, TYPES - 1).astype(jnp.int32),
        "counts": plant(jax.random.randint(key_of[2], (NX, NY, NZ), ATOMS_CELL // 2, ATOMS_CELL + 1), jax.random.fold_in(key_of[2], 1), ATOMS_CELL // 2, ATOMS_CELL).astype(jnp.int32),
        "type_charge": jnp.clip(jax.random.uniform(key_of[3], (TYPES,), jnp.float32, -1.0, 1.0), -1.0, 1.0),
        "type_sigma": jnp.clip(jnp.exp(jax.random.uniform(key_of[4], (TYPES,), jnp.float32, math.log(0.2), math.log(0.35))), 0.2, 0.35),
        "type_epsilon": jnp.clip(jnp.exp(jax.random.uniform(key_of[5], (TYPES,), jnp.float32, math.log(0.05), math.log(0.5))), 0.05, 0.5),
    }


soft_core = 0.09
corner_pairs = [(first_corner, second_corner) for first_corner in range(8) for second_corner in range(8) if first_corner & second_corner == 0 and first_corner <= second_corner]

def corner_of(which):
    return (which & 1, which >> 1 & 1, which >> 2 & 1)

def atom_table(positions, type_ids, counts, type_charge, type_sigma, type_epsilon):
    type_count = type_charge.shape[0]
    kinds_shape = (type_count, 1, 1, 1, 1)
    onehot = (type_ids[None] == jnp.arange(type_count, dtype=jnp.int32).reshape(kinds_shape)).astype(jnp.float32)
    charge = lax.optimization_barrier(jnp.sum(onehot * type_charge.reshape(kinds_shape), 0))
    sigma_atom = lax.optimization_barrier(jnp.sum(onehot * type_sigma.reshape(kinds_shape), 0))
    depth_atom = lax.optimization_barrier(jnp.sum(onehot * jnp.sqrt(type_epsilon).reshape(kinds_shape), 0))
    slots = lax.broadcasted_iota(jnp.int32, type_ids.shape, 3)
    occupied = (slots < counts[..., None]).astype(jnp.float32)
    return jnp.stack([positions[0], positions[1], positions[2], charge, sigma_atom, depth_atom, occupied])

def pair_terms(first, second, offset, selfpair):
    displace = second[:3, :, None, :] - first[:3, :, :, None] + offset[:, None, None, None]
    dist_sq = lax.optimization_barrier(jnp.sum(displace * displace, 0))
    width_atoms = first.shape[-1]
    live_mask = first[6][:, :, None] * second[6][:, None, :] * (dist_sq < 1.0).astype(jnp.float32)
    if selfpair:
        ordered = (lax.broadcasted_iota(jnp.int32, (width_atoms, width_atoms), 0) < lax.broadcasted_iota(jnp.int32, (width_atoms, width_atoms), 1)).astype(jnp.float32)
        live_mask = live_mask * ordered[None]
    sigma_pair = 0.5 * (first[4][:, :, None] + second[4][:, None, :])
    depth_pair = first[5][:, :, None] * second[5][:, None, :]
    coulomb = first[3][:, :, None] * second[3][:, None, :]
    soft_sq = dist_sq + soft_core
    inverse = lax.rsqrt(soft_sq)
    ratio_six = (sigma_pair * sigma_pair / soft_sq) ** 3
    ratio_twelve = ratio_six * ratio_six
    value_here = 4.0 * depth_pair * (ratio_twelve - ratio_six) + coulomb * inverse
    slope_here = (4.0 * depth_pair * (6.0 * ratio_six - 12.0 * ratio_twelve) - coulomb * inverse) * inverse
    cut_sq = 1.0 + soft_core
    cut_len = cut_sq ** 0.5
    cut_six = (sigma_pair * sigma_pair / cut_sq) ** 3
    cut_twelve = cut_six * cut_six
    value_cut = 4.0 * depth_pair * (cut_twelve - cut_six) + coulomb / cut_len
    slope_cut = (4.0 * depth_pair * (6.0 * cut_six - 12.0 * cut_twelve) - coulomb / cut_len) / cut_len
    energy = live_mask * (value_here - value_cut - (soft_sq * inverse - cut_len) * slope_cut)
    slope = live_mask * (slope_here - slope_cut) * inverse
    weighted = slope[None] * displace
    return (lax.optimization_barrier(jnp.sum(weighted, 3)), -lax.optimization_barrier(jnp.sum(weighted, 2)), jnp.sum(energy), jnp.sum(slope * dist_sq))

def reference(positions, type_ids, counts, type_charge, type_sigma, type_epsilon):
    features = atom_table(positions, type_ids, counts, type_charge, type_sigma, type_epsilon)
    forces = jnp.zeros((3, NX, NY, NZ, ATOMS_CELL), jnp.float32)
    energy = jnp.float32(0.0)
    virial = jnp.float32(0.0)

    def rows_of(which):
        shift_x, shift_y, shift_z = corner_of(which)
        shifted = jnp.roll(features, (-shift_x, -shift_y, -shift_z), (1, 2, 3))
        return jnp.transpose(shifted, (1, 2, 0, 3, 4)).reshape((NX * NY, 7, NZ, ATOMS_CELL))

    def placed(force_rows, which):
        shift_x, shift_y, shift_z = corner_of(which)
        grid = jnp.transpose(force_rows.reshape((NX, NY, 3, NZ, ATOMS_CELL)), (2, 0, 1, 3, 4))
        return jnp.roll(grid, (shift_x, shift_y, shift_z), (1, 2, 3))
    for first_corner, second_corner in corner_pairs:
        offset = jnp.array([float(a - b) for a, b in zip(corner_of(second_corner), corner_of(first_corner))], jnp.float32)
        selfpair = first_corner == second_corner

        def one_row(member, offset=offset, selfpair=selfpair):
            return pair_terms(member[0], member[1], offset, selfpair)
        force_first, force_second, energies, virials = lax.map(one_row, (rows_of(first_corner), rows_of(second_corner)))
        forces = forces + placed(force_first, first_corner) + placed(force_second, second_corner)
        energy = energy + jnp.sum(energies)
        virial = virial + jnp.sum(virials)
    normaliser = 1.0 / (NX * NY * NZ * ATOMS_CELL)
    return (forces, jnp.stack([energy, virial]) * normaliser)
```

```python
import functools

import jax
import jax.numpy as jnp
from jax import lax
from jax.experimental import pallas as pl
from jax.experimental.pallas import tpu as pltpu
from jax.sharding import PartitionSpec as P

MESH = pl.DeviceIdType.MESH
AXES = ("gx", "gy", "gz")
soft_core = 0.09
cut_sq = 1.0 + soft_core
cut_len = cut_sq**0.5
second_of = {0: (0, 1, 2, 3, 4, 5, 6, 7), 1: (2, 6), 2: (4, 5), 4: (1, 3)}
VMEM_LIMIT = 60 * 1024 * 1024


def corner_of(which):
    return (which & 1, which >> 1 & 1, which >> 2 & 1)


def neighbour(which, step):
    target = {}
    for axis, bit in zip(AXES, corner_of(which)):
        if bit:
            count = lax.axis_size(axis)
            target[axis] = lax.rem(lax.axis_index(axis) + step + count, count)
    return target


def halo_kernel(own, ext, send_sem, recv_sem):
    sizes = own.shape[:3]
    barrier = pltpu.get_barrier_semaphore()
    for which in range(1, 8):
        pl.semaphore_signal(barrier, inc=1, device_id=neighbour(which, 1), device_id_type=MESH)
    ext[: sizes[0], : sizes[1], : sizes[2]] = own[...]
    pl.semaphore_wait(barrier, 7)
    copies = []
    for which in range(1, 8):
        bits = corner_of(which)
        source = tuple(pl.ds(0, 1 if bit else size) for bit, size in zip(bits, sizes))
        target = tuple(
            pl.ds(size, 1) if bit else pl.ds(0, size) for bit, size in zip(bits, sizes)
        )
        copy = pltpu.make_async_remote_copy(
            src_ref=own.at[source],
            dst_ref=ext.at[target],
            send_sem=send_sem.at[which],
            recv_sem=recv_sem.at[which],
            device_id=neighbour(which, -1),
            device_id_type=MESH,
        )
        copy.start()
        copies.append(copy)
    for copy in copies:
        copy.wait()


def pair_kernel(types, ext, reaction, totals, rows, first, table, force_i, force_j):
    ext_sizes = ext.shape[:3]
    sizes = tuple(size - 1 for size in ext_sizes)
    width = ext.shape[-1]
    groups = width // 8
    per_cell = 3 + 5 * types
    cells = [
        (x, y, z)
        for x in range(ext_sizes[0])
        for y in range(ext_sizes[1])
        for z in range(ext_sizes[2])
    ]

    def index_of(x, y, z):
        return (x * ext_sizes[1] + y) * ext_sizes[2] + z

    pack = width // 4
    force_i[...] = jnp.zeros(force_i.shape, jnp.float32)
    force_j[...] = jnp.zeros(force_j.shape, jnp.float32)
    row_at = lax.broadcasted_iota(jnp.int32, (4, width), 0)
    for cell, (x, y, z) in enumerate(cells):
        base = jnp.where(row_at == 0, x, jnp.where(row_at == 1, y, jnp.where(row_at == 2, z, 0)))
        values = ext[x, y, z, 0:4] + base.astype(jnp.float32)
        for axis in range(3):
            table[cell, axis] = jnp.broadcast_to(values[axis : axis + 1], (8, width))
        parked = (row_at == 0) & (values[3:4] < 0.0)
        rows[pl.ds(4 * cell, 4)] = jnp.where(parked, x + 4.0, values)
        for kind in range(types):
            line = [
                jnp.broadcast_to(ext[x, y, z, pl.ds(4 + 4 * kind + at, 1)], (8, width))
                for at in range(4)
            ]
            for at in range(4):
                table[cell, 3 + 5 * kind + at] = line[at]
            table[cell, 3 + 5 * kind + 4] = cut_len * line[3] - (
                line[0] * (cut_sq**-6 / 12.0) - line[1] * (cut_sq**-3 / 6.0) + line[2] / cut_len
            )
    for cell, (x, y, z) in enumerate(cells):
        if cell % pack == 0:
            turned = jnp.transpose(rows[pl.ds(4 * cell, width)])
        if (x == sizes[0]) + (y == sizes[1]) + (z == sizes[2]) > 1:
            continue
        for axis in range(4):
            lane = 4 * (cell % pack) + axis
            first[cell, axis] = jnp.broadcast_to(
                turned[:, lane : lane + 1], (width, width)
            ).reshape((groups, 8, width))

    def interact(own, other, kinds, depth, ordered=None):
        xi, yi, zi = own
        second = [table[other, at][None] for at in range(per_cell)]

        def chosen(at):
            value = second[3 + at]
            for kind in range(1, types):
                value = jnp.where(kinds[kind - 1], second[3 + 5 * kind + at], value)
            return value

        dx, dy, dz = second[0] - xi, second[1] - yi, second[2] - zi
        soft_sq = jnp.minimum(dx * dx + dy * dy + dz * dz + soft_core, cut_sq)
        inverse = lax.rsqrt(soft_sq)
        inverse_2 = inverse * inverse
        inverse_6 = inverse_2 * inverse_2 * inverse_2
        twelve = chosen(0) * inverse_6 * inverse_6
        six = chosen(1) * inverse_6
        coulomb = chosen(2) * inverse
        shift = chosen(3) * (soft_sq * inverse)
        slope = ((six - twelve) - (coulomb + shift)) * inverse_2
        forces = (slope * dx, slope * dy, slope * dz)
        if ordered is None:
            for axis in range(3):
                force_j[other, axis] -= jnp.sum(forces[axis], 0)
            return forces, (twelve, six, coulomb, shift)
        value = twelve * (1.0 / 12.0) - six * (1.0 / 6.0) + coulomb - shift + chosen(4)
        return forces, jnp.sum(jnp.where(ordered, value, 0.0), 0)

    def one_cell(member, energy):
        z0 = lax.rem(member, sizes[2])
        y0 = lax.rem(member // sizes[2], sizes[1])
        x0 = member // (sizes[2] * sizes[1])

        def cell_at(which):
            shift = corner_of(which)
            return index_of(x0 + shift[0], y0 + shift[1], z0 + shift[2])

        for first_corner, seconds in second_of.items():
            depth = 2 if first_corner == 0 else 4
            here = cell_at(first_corner)
            others = [cell_at(which) for which in seconds]
            kind_row = rows[pl.ds(4 * here + 3, 1)]
            held = jnp.sum((kind_row >= 0.0).astype(jnp.int32))
            trips = (held + (8 * depth - 1)) // (8 * depth)
            tile = here // pack
            lane_at = lax.broadcasted_iota(jnp.int32, (1, 8, width), 2) - 4 * lax.rem(here, pack)
            slot_at = (
                lax.broadcasted_iota(jnp.int32, (depth, 8, width), 0) * 8
                + lax.broadcasted_iota(jnp.int32, (depth, 8, width), 1)
                - lax.broadcasted_iota(jnp.int32, (depth, 8, width), 2)
            )

            def step(at, carry, first_corner=first_corner, seconds=seconds, depth=depth,
                     here=here, others=others, tile=tile, lane_at=lane_at, slot_at=slot_at):
                energy, numbers = carry[0], list(carry[1:])
                span = pl.ds(at * depth, depth)
                own = tuple(first[here, axis, span] for axis in range(3))
                kind_at = first[here, 3, span]
                kinds = [kind_at == float(kind) for kind in range(1, types)]
                numbers = [
                    number + jnp.sum(kind.astype(jnp.float32), 0)
                    for number, kind in zip(numbers, kinds)
                ]
                total = None
                sums = None
                for which, other in zip(seconds, others):
                    if which == first_corner:
                        forces, own_energy = interact(
                            own, other, kinds, depth, slot_at + at * (8 * depth) < 0
                        )
                        energy = energy + own_energy
                    else:
                        forces, terms = interact(own, other, kinds, depth)
                        terms = [jnp.sum(term, 0) for term in terms]
                        sums = terms if sums is None else [a + b for a, b in zip(sums, terms)]
                    total = forces if total is None else [a + b for a, b in zip(total, forces)]
                energy = energy + (
                    (sums[0] * (1.0 / 12.0) - sums[1] * (1.0 / 6.0)) + (sums[2] - sums[3])
                )
                summed = [jnp.sum(value, 2, keepdims=True) for value in total]
                placed = jnp.where(
                    lane_at == 0,
                    summed[0],
                    jnp.where(
                        lane_at == 1, summed[1], jnp.where(lane_at == 2, summed[2], 0.0)
                    ),
                )
                force_i[tile, span] += placed
                return (energy, *numbers)

            zero = jnp.zeros((8, width), jnp.float32)
            energy, *numbers = lax.fori_loop(
                0, trips, step, (energy,) + (zero,) * (types - 1)
            )
            rest = jnp.full((8, width), (trips * depth).astype(jnp.float32))
            for number in numbers:
                rest = rest - number
            for which, other in zip(seconds, others):
                if which != first_corner:
                    for kind, number in enumerate([rest, *numbers]):
                        energy = energy + number * table[other, 3 + 5 * kind + 4]
        return energy

    members = sizes[0] * sizes[1] * sizes[2]
    energy = lax.fori_loop(0, members, one_cell, jnp.zeros((8, width), jnp.float32))

    virial = jnp.zeros((3, width), jnp.float32)
    turned = None
    reaction[...] = jnp.zeros(reaction.shape, jnp.float32)
    for cell, (x, y, z) in enumerate(cells):
        if cell % pack == 0:
            turned = jnp.transpose(force_i[cell // pack].reshape((width, width)))
        lane = 4 * (cell % pack)
        second_sum = jnp.concatenate(
            [jnp.sum(force_j[cell, axis], 0, keepdims=True) for axis in range(3)], 0
        )
        held = rows[pl.ds(4 * cell + 3, 1)] >= 0.0
        force = jnp.where(held, turned[lane : lane + 3] + second_sum, 0.0)
        reaction[x, y, z, 0:3] = force
        virial = virial - force * rows[pl.ds(4 * cell, 3)]
    totals[...] = jnp.zeros(totals.shape, jnp.float32)
    totals[0:1] = jnp.sum(energy, 0, keepdims=True)
    totals[1:2] = jnp.sum(virial, 0, keepdims=True)


def return_kernel(
    normaliser, reaction, part, forces, totals, *scratch
):
    ext_sizes = reaction.shape[:3]
    sizes = tuple(size - 1 for size in ext_sizes)
    landed = scratch[:7]
    send_sem, recv_sem, line, plane, middle, line_send, line_recv, plane_send, plane_recv = scratch[7:]
    count_x, count_y, count_z = (lax.axis_size(axis) for axis in AXES)
    at_x, at_y, at_z = (lax.axis_index(axis) for axis in AXES)
    count_plane = count_y * count_z
    at_plane = at_y * count_z + at_z

    def line_target(step):
        return {"gx": lax.rem(at_x + step, count_x)}

    def plane_target(step):
        spot = lax.rem(at_plane + step, count_plane)
        return {"gy": spot // count_z, "gz": lax.rem(spot, count_z)}

    barrier = pltpu.get_barrier_semaphore()
    for which in range(1, 8):
        pl.semaphore_signal(barrier, inc=1, device_id=neighbour(which, -1), device_id_type=MESH)
    for step in range(1, count_x):
        pl.semaphore_signal(barrier, inc=1, device_id=line_target(step), device_id_type=MESH)
    for step in range(1, count_plane):
        pl.semaphore_signal(barrier, inc=1, device_id=plane_target(step), device_id_type=MESH)
    pl.semaphore_wait(barrier, 7 + count_x - 1 + count_plane - 1)

    copies = []
    for which in range(1, 8):
        source = tuple(
            pl.ds(size, 1) if bit else pl.ds(0, size)
            for bit, size in zip(corner_of(which), sizes)
        )
        copy = pltpu.make_async_remote_copy(
            src_ref=reaction.at[source],
            dst_ref=landed[which - 1],
            send_sem=send_sem.at[which],
            recv_sem=recv_sem.at[which],
            device_id=neighbour(which, 1),
            device_id_type=MESH,
        )
        copy.start()
        copies.append(copy)
    line_copies = []
    for step in range(1, count_x):
        copy = pltpu.make_async_remote_copy(
            src_ref=part,
            dst_ref=line.at[at_x],
            send_sem=line_send.at[step],
            recv_sem=line_recv.at[step],
            device_id=line_target(step),
            device_id_type=MESH,
        )
        copy.start()
        line_copies.append(copy)
    line[at_x] = part[...]
    for copy in line_copies:
        copy.wait()
    summed = line[0]
    for step in range(1, count_x):
        summed = summed + line[step]
    middle[...] = summed
    plane[at_plane] = summed
    for copy in copies:
        copy.wait()
    for x in range(sizes[0]):
        for y in range(sizes[1]):
            for z in range(sizes[2]):
                value = reaction[x, y, z]
                for which in range(1, 8):
                    bits = corner_of(which)
                    spot = (x, y, z)
                    if all(not bit or at == 0 for bit, at in zip(bits, spot)):
                        value = value + landed[which - 1][
                            tuple(0 if bit else at for bit, at in zip(bits, spot))
                        ]
                for axis in range(3):
                    forces[axis, x, y, pl.ds(z, 1)] = value[axis : axis + 1]
    plane_copies = []
    for step in range(1, count_plane):
        copy = pltpu.make_async_remote_copy(
            src_ref=middle,
            dst_ref=plane.at[at_plane],
            send_sem=plane_send.at[step],
            recv_sem=plane_recv.at[step],
            device_id=plane_target(step),
            device_id_type=MESH,
        )
        copy.start()
        plane_copies.append(copy)
    for copy in plane_copies:
        copy.wait()
    summed = plane[0]
    for step in range(1, count_plane):
        summed = summed + plane[step]
    totals[0] = jnp.sum(summed[0:1]) * normaliser
    totals[1] = jnp.sum(summed[1:2]) * normaliser


def packed_rows(positions, type_ids, counts, type_charge, type_sigma, type_epsilon):
    types = type_charge.shape[0]
    shape = type_ids.shape
    occupied = lax.broadcasted_iota(jnp.int32, shape, 3) < counts[..., None]
    root = jnp.sqrt(type_epsilon)

    def of_type(values):
        picked = jnp.broadcast_to(values[0], shape)
        for kind in range(1, types):
            picked = jnp.where(type_ids == kind, values[kind], picked)
        return picked

    lines = [positions[0], positions[1], positions[2]]
    lines.append(jnp.where(occupied, type_ids.astype(jnp.float32), -1.0))
    for kind in range(types):
        sigma_pair = 0.5 * (type_sigma + type_sigma[kind])
        depth_pair = 4.0 * root * root[kind]
        coulomb = type_charge * type_charge[kind]
        sig_six = (sigma_pair * sigma_pair) ** 3
        six = 6.0 * depth_pair * sig_six
        twelve = 12.0 * depth_pair * sig_six * sig_six
        shift = ((six * cut_sq**-3 - twelve * cut_sq**-6) - coulomb / cut_len) / cut_len
        for values in (twelve, six, coulomb, shift):
            lines.append(jnp.where(occupied, of_type(values), 0.0))
    count = -(-len(lines) // 8) * 8
    lines += [jnp.zeros(shape, jnp.float32)] * (count - len(lines))
    return jnp.stack(lines, 3)


def per_device(positions, type_ids, counts, type_charge, type_sigma, type_epsilon):
    types = type_charge.shape[0]
    own = packed_rows(positions, type_ids, counts, type_charge, type_sigma, type_epsilon)
    sizes, (height, width) = own.shape[:3], own.shape[3:]
    ext_sizes = tuple(size + 1 for size in sizes)
    cells = ext_sizes[0] * ext_sizes[1] * ext_sizes[2]
    vmem = pl.BlockSpec(memory_space=pltpu.VMEM)
    smem = pl.BlockSpec(memory_space=pltpu.SMEM)
    f32 = jnp.float32
    ext = pl.pallas_call(
        halo_kernel,
        name="halo",
        out_shape=jax.ShapeDtypeStruct(ext_sizes + (height, width), f32),
        in_specs=[vmem],
        out_specs=vmem,
        scratch_shapes=[pltpu.SemaphoreType.DMA((8,)), pltpu.SemaphoreType.DMA((8,))],
        compiler_params=pltpu.CompilerParams(collective_id=0, has_side_effects=True),
    )(own)
    pack = width // 4
    tiles = -(-cells // pack)
    reaction, part = pl.pallas_call(
        functools.partial(pair_kernel, types),
        name="pairs",
        out_shape=(
            jax.ShapeDtypeStruct(ext_sizes + (8, width), f32),
            jax.ShapeDtypeStruct((8, width), f32),
        ),
        in_specs=[vmem],
        out_specs=(vmem, vmem),
        scratch_shapes=[
            pltpu.VMEM((tiles * width, width), f32),
            pltpu.VMEM((cells, 4, width // 8, 8, width), f32),
            pltpu.VMEM((cells, 3 + 5 * types, 8, width), f32),
            pltpu.VMEM((tiles, width // 8, 8, width), f32),
            pltpu.VMEM((cells, 3, 8, width), f32),
        ],
        compiler_params=pltpu.CompilerParams(vmem_limit_bytes=VMEM_LIMIT),
    )(ext)
    count_x, count_y, count_z = (lax.axis_size(axis) for axis in AXES)
    count_plane = count_y * count_z
    normaliser = 1.0 / (
        sizes[0] * count_x * sizes[1] * count_y * sizes[2] * count_z * width
    )
    landing = [
        pltpu.VMEM(
            tuple(1 if bit else size for bit, size in zip(corner_of(which), sizes)) + (8, width),
            f32,
        )
        for which in range(1, 8)
    ]
    forces, totals = pl.pallas_call(
        functools.partial(return_kernel, normaliser),
        name="giveback",
        out_shape=(
            jax.ShapeDtypeStruct((3,) + sizes + (width,), f32),
            jax.ShapeDtypeStruct((2,), f32),
        ),
        in_specs=[vmem, vmem],
        out_specs=(vmem, smem),
        scratch_shapes=landing
        + [
            pltpu.SemaphoreType.DMA((8,)),
            pltpu.SemaphoreType.DMA((8,)),
            pltpu.VMEM((count_x, 8, width), f32),
            pltpu.VMEM((count_plane, 8, width), f32),
            pltpu.VMEM((8, width), f32),
            pltpu.SemaphoreType.DMA((count_x,)),
            pltpu.SemaphoreType.DMA((count_x,)),
            pltpu.SemaphoreType.DMA((count_plane,)),
            pltpu.SemaphoreType.DMA((count_plane,)),
        ],
        compiler_params=pltpu.CompilerParams(collective_id=1, has_side_effects=True),
    )(reaction, part)
    return forces, totals


def solution(mesh):
    in_specs = (
        P(None, "gx", "gy", "gz", None),
        P("gx", "gy", "gz", None),
        P("gx", "gy", "gz"),
        P(),
        P(),
        P(),
    )
    out_specs = (P(None, "gx", "gy", "gz", None), P())
    return jax.shard_map(
        per_device, mesh=mesh, in_specs=in_specs, out_specs=out_specs, check_vma=False
    )
```

```python
import functools

import jax
import jax.numpy as jnp
from jax import lax
from jax.experimental import pallas as pl
from jax.experimental.pallas import tpu as pltpu
from jax.sharding import PartitionSpec as P

MESH = pl.DeviceIdType.MESH
AXES = ("gx", "gy", "gz")
soft_core = 0.09
cut_sq = 1.0 + soft_core
cut_len = cut_sq**0.5
second_of = {0: (0, 1, 2, 3, 4, 5, 6, 7), 1: (2, 6), 2: (4, 5), 4: (1, 3)}
VMEM_LIMIT = 40 * 1024 * 1024


def corner_of(which):
    return (which & 1, which >> 1 & 1, which >> 2 & 1)


def neighbour(which, step):
    target = {}
    for axis, bit in zip(AXES, corner_of(which)):
        if bit:
            count = lax.axis_size(axis)
            target[axis] = lax.rem(lax.axis_index(axis) + step + count, count)
    return target


def halo_kernel(positions, type_ids, counts, ext, own, send_sem, recv_sem):
    sizes = own.shape[:3]
    width = own.shape[-1]
    barrier = pltpu.get_barrier_semaphore()
    for which in range(1, 8):
        pl.semaphore_signal(barrier, inc=1, device_id=neighbour(which, 1), device_id_type=MESH)
    slot = lax.broadcasted_iota(jnp.int32, (1, width), 1)
    blank = jnp.zeros((4, width), jnp.float32)
    for x in range(sizes[0]):
        for y in range(sizes[1]):
            for z in range(sizes[2]):
                kind = type_ids[x, y, pl.ds(z, 1)].astype(jnp.float32)
                lines = [positions[axis, x, y, pl.ds(z, 1)] for axis in range(3)]
                lines.append(jnp.where(slot < counts[x, y, z], kind, -1.0))
                tile = jnp.concatenate(lines + [blank], 0)
                own[x, y, z] = tile
                ext[x, y, z] = tile
    pl.semaphore_wait(barrier, 7)
    copies = []
    for which in range(1, 8):
        bits = corner_of(which)
        source = tuple(pl.ds(0, 1 if bit else size) for bit, size in zip(bits, sizes))
        target = tuple(
            pl.ds(size, 1) if bit else pl.ds(0, size) for bit, size in zip(bits, sizes)
        )
        copy = pltpu.make_async_remote_copy(
            src_ref=own.at[source],
            dst_ref=ext.at[target],
            send_sem=send_sem.at[which],
            recv_sem=recv_sem.at[which],
            device_id=neighbour(which, -1),
            device_id_type=MESH,
        )
        copy.start()
        copies.append(copy)
    for copy in copies:
        copy.wait()


def type_tables(types, shape, charges, sigmas, epsilons):
    def full(value):
        return jnp.full(shape, value, jnp.float32)

    charge = [full(charges[kind]) for kind in range(types)]
    sigma = [full(sigmas[kind]) for kind in range(types)]
    root = [jnp.sqrt(full(epsilons[kind])) for kind in range(types)]
    tables = {}
    for a in range(types):
        for b in range(types):
            sigma_pair = 0.5 * (sigma[a] + sigma[b])
            depth_pair = 4.0 * root[a] * root[b]
            coulomb = charge[a] * charge[b]
            square = sigma_pair * sigma_pair
            sig_six = square * square * square
            six = 6.0 * depth_pair * sig_six
            twelve = 12.0 * depth_pair * sig_six * sig_six
            cut_six, cut_twelve, cut_coulomb = six * cut_sq**-3, twelve * cut_sq**-6, coulomb / cut_len
            shift = ((cut_six - cut_twelve) - cut_coulomb) / cut_len
            level = cut_len * shift - (cut_twelve / 12.0 - cut_six / 6.0 + cut_coulomb)
            tables[a, b] = (twelve, six, coulomb, shift, level)
    return tables


def pair_kernel(
    types, charges, sigmas, epsilons, ext, reaction, totals,
    rows, first, table, force_i, force_j, held_of,
):
    ext_sizes = ext.shape[:3]
    sizes = tuple(size - 1 for size in ext_sizes)
    width = ext.shape[-1]
    groups = width // 8
    per_cell = 3 + 5 * types
    cells = [
        (x, y, z)
        for x in range(ext_sizes[0])
        for y in range(ext_sizes[1])
        for z in range(ext_sizes[2])
    ]

    def index_of(x, y, z):
        return (x * ext_sizes[1] + y) * ext_sizes[2] + z

    pack = width // 4
    force_j[...] = jnp.zeros(force_j.shape, jnp.float32)
    row_at = lax.broadcasted_iota(jnp.int32, (4, width), 0)
    tables = type_tables(types, (8, width), charges, sigmas, epsilons)
    for cell, (x, y, z) in enumerate(cells):
        base = jnp.where(row_at == 0, x, jnp.where(row_at == 1, y, jnp.where(row_at == 2, z, 0)))
        values = ext[x, y, z, 0:4] + base.astype(jnp.float32)
        held_of[cell] = jnp.sum((values[3:4] >= 0.0).astype(jnp.int32))
        for axis in range(3):
            table[cell, axis] = jnp.broadcast_to(values[axis : axis + 1], (8, width))
        parked = (row_at == 0) & (values[3:4] < 0.0)
        rows[pl.ds(4 * cell, 4)] = jnp.where(parked, x + 4.0, values)
        kind_row = jnp.broadcast_to(values[3:4], (8, width))
        same = [kind_row == float(kind) for kind in range(types)]
        for kind in range(types):
            for at in range(5):
                picked = jnp.zeros((8, width), jnp.float32)
                for second_kind in range(types):
                    picked = jnp.where(same[second_kind], tables[kind, second_kind][at], picked)
                table[cell, 3 + 5 * kind + at] = picked
    for cell, (x, y, z) in enumerate(cells):
        if cell % pack == 0:
            turned = jnp.transpose(rows[pl.ds(4 * cell, width)])
        if (x == sizes[0]) + (y == sizes[1]) + (z == sizes[2]) > 1:
            continue
        for axis in range(4):
            lane = 4 * (cell % pack) + axis
            first[cell, axis] = jnp.broadcast_to(
                turned[:, lane : lane + 1], (width, width)
            ).reshape((groups, 8, width))

    def interact(own, other, kinds, depth, ordered=None):
        xi, yi, zi = own
        second = [table[other, at][None] for at in range(per_cell)]

        def chosen(at):
            value = second[3 + at]
            for kind in range(1, types):
                value = jnp.where(kinds[kind - 1], second[3 + 5 * kind + at], value)
            return value

        dx, dy, dz = second[0] - xi, second[1] - yi, second[2] - zi
        soft_sq = jnp.minimum(dx * dx + dy * dy + dz * dz + soft_core, cut_sq)
        inverse = lax.rsqrt(soft_sq)
        inverse_2 = inverse * inverse
        inverse_6 = inverse_2 * inverse_2 * inverse_2
        twelve = chosen(0) * inverse_6 * inverse_6
        six = chosen(1) * inverse_6
        coulomb = chosen(2) * inverse
        shift = chosen(3) * (soft_sq * inverse)
        slope = ((six - twelve) - (coulomb + shift)) * inverse_2
        forces = (slope * dx, slope * dy, slope * dz)
        if ordered is None:
            for axis in range(3):
                force_j[other, axis] -= jnp.sum(forces[axis], 0)
            return forces, (twelve, six, coulomb, shift)
        value = twelve * (1.0 / 12.0) - six * (1.0 / 6.0) + coulomb - shift + chosen(4)
        return forces, jnp.sum(jnp.where(ordered, value, 0.0), 0)

    def one_cell(member, energy):
        z0 = lax.rem(member, sizes[2])
        y0 = lax.rem(member // sizes[2], sizes[1])
        x0 = member // (sizes[2] * sizes[1])

        def cell_at(which):
            shift = corner_of(which)
            return index_of(x0 + shift[0], y0 + shift[1], z0 + shift[2])

        for first_corner, seconds in second_of.items():
            depth = 2 if first_corner == 0 else 4
            here = cell_at(first_corner)
            others = [cell_at(which) for which in seconds]
            trips = (held_of[here] + (8 * depth - 1)) // (8 * depth)
            part_at = tuple(second_of).index(first_corner)
            slot_at = (
                lax.broadcasted_iota(jnp.int32, (depth, 8, width), 0) * 8
                + lax.broadcasted_iota(jnp.int32, (depth, 8, width), 1)
                - lax.broadcasted_iota(jnp.int32, (depth, 8, width), 2)
            )

            def step(at, carry, first_corner=first_corner, seconds=seconds, depth=depth,
                     here=here, others=others, part_at=part_at, slot_at=slot_at):
                energy, numbers = carry[0], list(carry[1:])
                span = pl.ds(at * depth, depth)
                own = tuple(first[here, axis, span] for axis in range(3))
                kind_at = first[here, 3, span]
                kinds = [kind_at == float(kind) for kind in range(1, types)]
                numbers = [
                    number + jnp.sum(kind.astype(jnp.float32), 0)
                    for number, kind in zip(numbers, kinds)
                ]
                total = None
                sums = None
                for which, other in zip(seconds, others):
                    if which == first_corner:
                        forces, own_energy = interact(
                            own, other, kinds, depth, slot_at + at * (8 * depth) < 0
                        )
                        energy = energy + own_energy
                    else:
                        forces, terms = interact(own, other, kinds, depth)
                        terms = [jnp.sum(term, 0) for term in terms]
                        sums = terms if sums is None else [a + b for a, b in zip(sums, terms)]
                    total = forces if total is None else [a + b for a, b in zip(total, forces)]
                energy = energy + (
                    (sums[0] * (1.0 / 12.0) - sums[1] * (1.0 / 6.0)) + (sums[2] - sums[3])
                )
                for axis in range(3):
                    force_i[part_at, member, axis, span] = total[axis]
                return (energy, *numbers)

            zero = jnp.zeros((8, width), jnp.float32)
            energy, *numbers = lax.fori_loop(
                0, trips, step, (energy,) + (zero,) * (types - 1)
            )
            rest = jnp.full((8, width), (trips * depth).astype(jnp.float32))
            for number in numbers:
                rest = rest - number
            for which, other in zip(seconds, others):
                if which != first_corner:
                    for kind, number in enumerate([rest, *numbers]):
                        energy = energy + number * table[other, 3 + 5 * kind + 4]
        return energy

    members = sizes[0] * sizes[1] * sizes[2]
    energy = lax.fori_loop(0, members, one_cell, jnp.zeros((8, width), jnp.float32))

    virial = jnp.zeros((3, width), jnp.float32)
    ones = jnp.ones((8, 2 * width), jnp.bfloat16)
    reaction[...] = jnp.zeros(reaction.shape, jnp.float32)
    for cell, (x, y, z) in enumerate(cells):
        held = rows[pl.ds(4 * cell + 3, 1)] >= 0.0
        lines = []
        for axis in range(3):
            line = jnp.sum(force_j[cell, axis], 0, keepdims=True)
            partial = None
            for part_at, first_corner in enumerate(second_of):
                spot = [at - bit for at, bit in zip((x, y, z), corner_of(first_corner))]
                if all(0 <= at < size for at, size in zip(spot, sizes)):
                    member = (spot[0] * sizes[1] + spot[1]) * sizes[2] + spot[2]
                    value = force_i[part_at, member, axis].reshape((width, width))
                    partial = value if partial is None else partial + value
            if partial is not None:
                high = partial.astype(jnp.bfloat16)
                low = (partial - high.astype(jnp.float32)).astype(jnp.bfloat16)
                summed = lax.dot_general(
                    ones,
                    jnp.concatenate([high, low], 1),
                    (((1,), (1,)), ((), ())),
                    preferred_element_type=jnp.float32,
                )
                line = line + summed[0:1]
            lines.append(jnp.where(held, line, 0.0))
        force = jnp.concatenate(lines, 0)
        reaction[x, y, z, 0:3] = force
        virial = virial - force * rows[pl.ds(4 * cell, 3)]
    totals[...] = jnp.zeros(totals.shape, jnp.float32)
    totals[0:1] = jnp.sum(energy, 0, keepdims=True)
    totals[1:2] = jnp.sum(virial, 0, keepdims=True)


def return_kernel(
    normaliser, reaction, part, forces, totals, *scratch
):
    ext_sizes = reaction.shape[:3]
    sizes = tuple(size - 1 for size in ext_sizes)
    landed = scratch[:7]
    send_sem, recv_sem, line, plane, middle, line_send, line_recv, plane_send, plane_recv = scratch[7:]
    count_x, count_y, count_z = (lax.axis_size(axis) for axis in AXES)
    at_x, at_y, at_z = (lax.axis_index(axis) for axis in AXES)
    count_plane = count_y * count_z
    at_plane = at_y * count_z + at_z

    def line_target(step):
        return {"gx": lax.rem(at_x + step, count_x)}

    def plane_target(step):
        spot = lax.rem(at_plane + step, count_plane)
        return {"gy": spot // count_z, "gz": lax.rem(spot, count_z)}

    barrier = pltpu.get_barrier_semaphore()
    for which in range(1, 8):
        pl.semaphore_signal(barrier, inc=1, device_id=neighbour(which, -1), device_id_type=MESH)
    for step in range(1, count_x):
        pl.semaphore_signal(barrier, inc=1, device_id=line_target(step), device_id_type=MESH)
    for step in range(1, count_plane):
        pl.semaphore_signal(barrier, inc=1, device_id=plane_target(step), device_id_type=MESH)
    pl.semaphore_wait(barrier, 7 + count_x - 1 + count_plane - 1)

    copies = []
    for which in range(1, 8):
        source = tuple(
            pl.ds(size, 1) if bit else pl.ds(0, size)
            for bit, size in zip(corner_of(which), sizes)
        )
        copy = pltpu.make_async_remote_copy(
            src_ref=reaction.at[source],
            dst_ref=landed[which - 1],
            send_sem=send_sem.at[which],
            recv_sem=recv_sem.at[which],
            device_id=neighbour(which, 1),
            device_id_type=MESH,
        )
        copy.start()
        copies.append(copy)
    line_copies = []
    for step in range(1, count_x):
        copy = pltpu.make_async_remote_copy(
            src_ref=part,
            dst_ref=line.at[at_x],
            send_sem=line_send.at[step],
            recv_sem=line_recv.at[step],
            device_id=line_target(step),
            device_id_type=MESH,
        )
        copy.start()
        line_copies.append(copy)
    line[at_x] = part[...]
    for copy in line_copies:
        copy.wait()
    summed = line[0]
    for step in range(1, count_x):
        summed = summed + line[step]
    middle[...] = summed
    plane[at_plane] = summed
    for copy in copies:
        copy.wait()
    for x in range(sizes[0]):
        for y in range(sizes[1]):
            for z in range(sizes[2]):
                value = reaction[x, y, z]
                for which in range(1, 8):
                    bits = corner_of(which)
                    spot = (x, y, z)
                    if all(not bit or at == 0 for bit, at in zip(bits, spot)):
                        value = value + landed[which - 1][
                            tuple(0 if bit else at for bit, at in zip(bits, spot))
                        ]
                for axis in range(3):
                    forces[axis, x, y, pl.ds(z, 1)] = value[axis : axis + 1]
    plane_copies = []
    for step in range(1, count_plane):
        copy = pltpu.make_async_remote_copy(
            src_ref=middle,
            dst_ref=plane.at[at_plane],
            send_sem=plane_send.at[step],
            recv_sem=plane_recv.at[step],
            device_id=plane_target(step),
            device_id_type=MESH,
        )
        copy.start()
        plane_copies.append(copy)
    for copy in plane_copies:
        copy.wait()
    summed = plane[0]
    for step in range(1, count_plane):
        summed = summed + plane[step]
    totals[0] = jnp.sum(summed[0:1]) * normaliser
    totals[1] = jnp.sum(summed[1:2]) * normaliser


def per_device(positions, type_ids, counts, type_charge, type_sigma, type_epsilon):
    types = type_charge.shape[0]
    sizes, width = type_ids.shape[:3], type_ids.shape[3]
    ext_sizes = tuple(size + 1 for size in sizes)
    cells = ext_sizes[0] * ext_sizes[1] * ext_sizes[2]
    vmem = pl.BlockSpec(memory_space=pltpu.VMEM)
    smem = pl.BlockSpec(memory_space=pltpu.SMEM)
    f32 = jnp.float32
    ext = pl.pallas_call(
        halo_kernel,
        name="halo",
        out_shape=jax.ShapeDtypeStruct(ext_sizes + (8, width), f32),
        in_specs=[vmem, vmem, smem],
        out_specs=vmem,
        scratch_shapes=[pltpu.VMEM(sizes + (8, width), f32), pltpu.SemaphoreType.DMA((8,)), pltpu.SemaphoreType.DMA((8,))],
        compiler_params=pltpu.CompilerParams(
            collective_id=0, has_side_effects=True, vmem_limit_bytes=8 * 1024 * 1024
        ),
    )(positions, type_ids, counts)
    pack = width // 4
    tiles = -(-cells // pack)
    reaction, part = pl.pallas_call(
        functools.partial(pair_kernel, types),
        name="pairs",
        out_shape=(
            jax.ShapeDtypeStruct(ext_sizes + (8, width), f32),
            jax.ShapeDtypeStruct((8, width), f32),
        ),
        in_specs=[smem, smem, smem, vmem],
        out_specs=(vmem, vmem),
        scratch_shapes=[
            pltpu.VMEM((tiles * width, width), f32),
            pltpu.VMEM((cells, 4, width // 8, 8, width), f32),
            pltpu.VMEM((cells, 3 + 5 * types, 8, width), f32),
            pltpu.VMEM(
                (len(second_of), sizes[0] * sizes[1] * sizes[2], 3, width // 8, 8, width), f32
            ),
            pltpu.VMEM((cells, 3, 8, width), f32),
            pltpu.SMEM((cells,), jnp.int32),
        ],
        compiler_params=pltpu.CompilerParams(vmem_limit_bytes=VMEM_LIMIT),
    )(type_charge, type_sigma, type_epsilon, ext)
    count_x, count_y, count_z = (lax.axis_size(axis) for axis in AXES)
    count_plane = count_y * count_z
    normaliser = 1.0 / (
        sizes[0] * count_x * sizes[1] * count_y * sizes[2] * count_z * width
    )
    landing = [
        pltpu.VMEM(
            tuple(1 if bit else size for bit, size in zip(corner_of(which), sizes)) + (8, width),
            f32,
        )
        for which in range(1, 8)
    ]
    forces, totals = pl.pallas_call(
        functools.partial(return_kernel, normaliser),
        name="giveback",
        out_shape=(
            jax.ShapeDtypeStruct((3,) + sizes + (width,), f32),
            jax.ShapeDtypeStruct((2,), f32),
        ),
        in_specs=[vmem, vmem],
        out_specs=(vmem, smem),
        scratch_shapes=landing
        + [
            pltpu.SemaphoreType.DMA((8,)),
            pltpu.SemaphoreType.DMA((8,)),
            pltpu.VMEM((count_x, 8, width), f32),
            pltpu.VMEM((count_plane, 8, width), f32),
            pltpu.VMEM((8, width), f32),
            pltpu.SemaphoreType.DMA((count_x,)),
            pltpu.SemaphoreType.DMA((count_x,)),
            pltpu.SemaphoreType.DMA((count_plane,)),
            pltpu.SemaphoreType.DMA((count_plane,)),
        ],
        compiler_params=pltpu.CompilerParams(
            collective_id=1, has_side_effects=True, vmem_limit_bytes=8 * 1024 * 1024
        ),
    )(reaction, part)
    return forces, totals


def solution(mesh):
    in_specs = (
        P(None, "gx", "gy", "gz", None),
        P("gx", "gy", "gz", None),
        P("gx", "gy", "gz"),
        P(),
        P(),
        P(),
    )
    out_specs = (P(None, "gx", "gy", "gz", None), P())
    return jax.shard_map(
        per_device, mesh=mesh, in_specs=in_specs, out_specs=out_specs, check_vma=False
    )
```

```python
import functools

import jax
import jax.numpy as jnp
from jax import lax
from jax.experimental import pallas as pl
from jax.experimental.pallas import tpu as pltpu
from jax.sharding import PartitionSpec as P

MESH = pl.DeviceIdType.MESH
AXES = ("gx", "gy", "gz")
soft_core = 0.09
cut_sq = 1.0 + soft_core
cut_len = cut_sq**0.5
second_of = {0: (0, 1, 2, 3, 4, 5, 6, 7), 1: (2, 6), 2: (4, 5), 4: (1, 3)}
direct_limit = 64
VMEM_LIMIT = 40 * 1024 * 1024


def corner_of(which):
    return (which & 1, which >> 1 & 1, which >> 2 & 1)


def neighbour(which, step):
    target = {}
    for axis, bit in zip(AXES, corner_of(which)):
        if bit:
            count = lax.axis_size(axis)
            target[axis] = lax.rem(lax.axis_index(axis) + step + count, count)
    return target


def halo_kernel(positions, type_ids, counts, ext, own, send_sem, recv_sem):
    sizes = own.shape[:3]
    width = own.shape[-1]
    barrier = pltpu.get_barrier_semaphore()
    for which in range(1, 8):
        pl.semaphore_signal(barrier, inc=1, device_id=neighbour(which, 1), device_id_type=MESH)
    slot = lax.broadcasted_iota(jnp.int32, (1, width), 1)
    blank = jnp.zeros((4, width), jnp.float32)
    for x in range(sizes[0]):
        for y in range(sizes[1]):
            for z in range(sizes[2]):
                kind = type_ids[x, y, pl.ds(z, 1)].astype(jnp.float32)
                lines = [positions[axis, x, y, pl.ds(z, 1)] for axis in range(3)]
                lines.append(jnp.where(slot < counts[x, y, z], kind, -1.0))
                tile = jnp.concatenate(lines + [blank], 0)
                own[x, y, z] = tile
                ext[x, y, z] = tile
    pl.semaphore_wait(barrier, 7)
    copies = []
    for which in range(1, 8):
        bits = corner_of(which)
        source = tuple(pl.ds(0, 1 if bit else size) for bit, size in zip(bits, sizes))
        target = tuple(
            pl.ds(size, 1) if bit else pl.ds(0, size) for bit, size in zip(bits, sizes)
        )
        copy = pltpu.make_async_remote_copy(
            src_ref=own.at[source],
            dst_ref=ext.at[target],
            send_sem=send_sem.at[which],
            recv_sem=recv_sem.at[which],
            device_id=neighbour(which, -1),
            device_id_type=MESH,
        )
        copy.start()
        copies.append(copy)
    for copy in copies:
        copy.wait()


def type_tables(types, shape, charges, sigmas, epsilons):
    def full(value):
        return jnp.full(shape, value, jnp.float32)

    charge = [full(charges[kind]) for kind in range(types)]
    sigma = [full(sigmas[kind]) for kind in range(types)]
    root = [jnp.sqrt(full(epsilons[kind])) for kind in range(types)]
    tables = {}
    for a in range(types):
        for b in range(types):
            sigma_pair = 0.5 * (sigma[a] + sigma[b])
            depth_pair = 4.0 * root[a] * root[b]
            coulomb = charge[a] * charge[b]
            square = sigma_pair * sigma_pair
            sig_six = square * square * square
            six = 6.0 * depth_pair * sig_six
            twelve = 12.0 * depth_pair * sig_six * sig_six
            cut_six, cut_twelve, cut_coulomb = six * cut_sq**-3, twelve * cut_sq**-6, coulomb / cut_len
            shift = ((cut_six - cut_twelve) - cut_coulomb) / cut_len
            level = cut_len * shift - (cut_twelve / 12.0 - cut_six / 6.0 + cut_coulomb)
            tables[a, b] = (twelve, six, coulomb, shift, level)
    return tables


def pair_kernel(
    types, charges, sigmas, epsilons, ext, reaction, totals,
    rows, first, table, force_i, force_j, held_of,
):
    ext_sizes = ext.shape[:3]
    sizes = tuple(size - 1 for size in ext_sizes)
    width = ext.shape[-1]
    groups = width // 8
    per_cell = 3 + 5 * types
    cells = [
        (x, y, z)
        for x in range(ext_sizes[0])
        for y in range(ext_sizes[1])
        for z in range(ext_sizes[2])
    ]

    def index_of(x, y, z):
        return (x * ext_sizes[1] + y) * ext_sizes[2] + z

    pack = width // 4
    force_j[...] = jnp.zeros(force_j.shape, jnp.float32)
    row_at = lax.broadcasted_iota(jnp.int32, (4, width), 0)
    tables = type_tables(types, (8, width), charges, sigmas, epsilons)
    for cell, (x, y, z) in enumerate(cells):
        base = jnp.where(row_at == 0, x, jnp.where(row_at == 1, y, jnp.where(row_at == 2, z, 0)))
        values = ext[x, y, z, 0:4] + base.astype(jnp.float32)
        held_of[cell] = jnp.sum((values[3:4] >= 0.0).astype(jnp.int32))
        for axis in range(3):
            table[cell, axis] = jnp.broadcast_to(values[axis : axis + 1], (8, width))
        parked = (row_at == 0) & (values[3:4] < 0.0)
        rows[pl.ds(4 * cell, 4)] = jnp.where(parked, x + 4.0, values)
        kind_row = jnp.broadcast_to(values[3:4], (8, width))
        same = [kind_row == float(kind) for kind in range(types)]
        for kind in range(types):
            for at in range(5):
                picked = jnp.zeros((8, width), jnp.float32)
                for second_kind in range(types):
                    picked = jnp.where(same[second_kind], tables[kind, second_kind][at], picked)
                table[cell, 3 + 5 * kind + at] = picked
    for cell, (x, y, z) in enumerate(cells):
        if cell % pack == 0:
            turned = jnp.transpose(rows[pl.ds(4 * cell, width)])
        if (x == sizes[0]) + (y == sizes[1]) + (z == sizes[2]) > 1:
            continue
        for axis in range(4):
            lane = 4 * (cell % pack) + axis
            first[cell, axis] = jnp.broadcast_to(
                turned[:, lane : lane + 1], (width, width)
            ).reshape((groups, 8, width))

    def interact(own, other, kinds, depth, ordered=None):
        xi, yi, zi = own
        second = [table[other, at][None] for at in range(per_cell)]

        def chosen(at):
            value = second[3 + at]
            for kind in range(1, types):
                value = jnp.where(kinds[kind - 1], second[3 + 5 * kind + at], value)
            return value

        dx, dy, dz = second[0] - xi, second[1] - yi, second[2] - zi
        soft_sq = jnp.minimum(dx * dx + dy * dy + dz * dz + soft_core, cut_sq)
        inverse = lax.rsqrt(soft_sq)
        inverse_2 = inverse * inverse
        inverse_6 = inverse_2 * inverse_2 * inverse_2
        twelve = chosen(0) * inverse_6 * inverse_6
        six = chosen(1) * inverse_6
        coulomb = chosen(2) * inverse
        shift = chosen(3) * (soft_sq * inverse)
        slope = ((six - twelve) - (coulomb + shift)) * inverse_2
        forces = (slope * dx, slope * dy, slope * dz)
        if ordered is None:
            for axis in range(3):
                force_j[other, axis] -= jnp.sum(forces[axis], 0)
            return forces, (twelve, six, coulomb, shift)
        value = twelve * (1.0 / 12.0) - six * (1.0 / 6.0) + coulomb - shift + chosen(4)
        return forces, jnp.sum(jnp.where(ordered, value, 0.0), 0)

    def one_cell(member, energy):
        z0 = lax.rem(member, sizes[2])
        y0 = lax.rem(member // sizes[2], sizes[1])
        x0 = member // (sizes[2] * sizes[1])

        def cell_at(which):
            shift = corner_of(which)
            return index_of(x0 + shift[0], y0 + shift[1], z0 + shift[2])

        for first_corner, seconds in second_of.items():
            depth = 2 if first_corner == 0 else 4
            here = cell_at(first_corner)
            others = [cell_at(which) for which in seconds]
            trips = (held_of[here] + (8 * depth - 1)) // (8 * depth)
            part_at = tuple(second_of).index(first_corner)
            slot_at = (
                lax.broadcasted_iota(jnp.int32, (depth, 8, width), 0) * 8
                + lax.broadcasted_iota(jnp.int32, (depth, 8, width), 1)
                - lax.broadcasted_iota(jnp.int32, (depth, 8, width), 2)
            )

            def step(at, carry, first_corner=first_corner, seconds=seconds, depth=depth,
                     here=here, others=others, part_at=part_at, slot_at=slot_at):
                energy, numbers = carry[0], list(carry[1:])
                span = pl.ds(at * depth, depth)
                own = tuple(first[here, axis, span] for axis in range(3))
                kind_at = first[here, 3, span]
                kinds = [kind_at == float(kind) for kind in range(1, types)]
                numbers = [
                    number + jnp.sum(kind.astype(jnp.float32), 0)
                    for number, kind in zip(numbers, kinds)
                ]
                total = None
                sums = None
                for which, other in zip(seconds, others):
                    if which == first_corner:
                        forces, own_energy = interact(
                            own, other, kinds, depth, slot_at + at * (8 * depth) < 0
                        )
                        energy = energy + own_energy
                    else:
                        forces, terms = interact(own, other, kinds, depth)
                        terms = [jnp.sum(term, 0) for term in terms]
                        sums = terms if sums is None else [a + b for a, b in zip(sums, terms)]
                    total = forces if total is None else [a + b for a, b in zip(total, forces)]
                energy = energy + (
                    (sums[0] * (1.0 / 12.0) - sums[1] * (1.0 / 6.0)) + (sums[2] - sums[3])
                )
                for axis in range(3):
                    force_i[part_at, member, axis, span] = total[axis]
                return (energy, *numbers)

            zero = jnp.zeros((8, width), jnp.float32)
            energy, *numbers = lax.fori_loop(
                0, trips, step, (energy,) + (zero,) * (types - 1)
            )
            rest = jnp.full((8, width), (trips * depth).astype(jnp.float32))
            for number in numbers:
                rest = rest - number
            for which, other in zip(seconds, others):
                if which != first_corner:
                    for kind, number in enumerate([rest, *numbers]):
                        energy = energy + number * table[other, 3 + 5 * kind + 4]
        return energy

    members = sizes[0] * sizes[1] * sizes[2]
    energy = lax.fori_loop(0, members, one_cell, jnp.zeros((8, width), jnp.float32))

    virial = jnp.zeros((3, width), jnp.float32)
    ones = jnp.ones((8, 2 * width), jnp.bfloat16)
    reaction[...] = jnp.zeros(reaction.shape, jnp.float32)
    for cell, (x, y, z) in enumerate(cells):
        held = rows[pl.ds(4 * cell + 3, 1)] >= 0.0
        lines = []
        for axis in range(3):
            line = jnp.sum(force_j[cell, axis], 0, keepdims=True)
            partial = None
            for part_at, first_corner in enumerate(second_of):
                spot = [at - bit for at, bit in zip((x, y, z), corner_of(first_corner))]
                if all(0 <= at < size for at, size in zip(spot, sizes)):
                    member = (spot[0] * sizes[1] + spot[1]) * sizes[2] + spot[2]
                    value = force_i[part_at, member, axis].reshape((width, width))
                    partial = value if partial is None else partial + value
            if partial is not None:
                high = partial.astype(jnp.bfloat16)
                low = (partial - high.astype(jnp.float32)).astype(jnp.bfloat16)
                summed = lax.dot_general(
                    ones,
                    jnp.concatenate([high, low], 1),
                    (((1,), (1,)), ((), ())),
                    preferred_element_type=jnp.float32,
                )
                line = line + summed[0:1]
            lines.append(jnp.where(held, line, 0.0))
        force = jnp.concatenate(lines, 0)
        reaction[x, y, z, 0:3] = force
        virial = virial - force * rows[pl.ds(4 * cell, 3)]
    totals[0:1] = jnp.sum(energy, 0, keepdims=True)
    totals[1:2] = jnp.sum(virial, 0, keepdims=True)


def return_kernel(
    normaliser, reaction, part, forces, totals, *scratch
):
    ext_sizes = reaction.shape[:3]
    sizes = tuple(size - 1 for size in ext_sizes)
    landed = scratch[:7]
    send_sem, recv_sem, line, plane, middle, line_send, line_recv, plane_send, plane_recv = scratch[7:]
    count_x, count_y, count_z = (lax.axis_size(axis) for axis in AXES)
    at_x, at_y, at_z = (lax.axis_index(axis) for axis in AXES)
    count_plane = count_y * count_z
    at_plane = at_y * count_z + at_z
    direct = count_x * count_plane <= direct_limit
    if direct:
        count_plane, at_plane = count_x * count_plane, at_x * count_plane + at_plane
        count_x, at_x = 1, 0

    def line_target(step):
        return {"gx": lax.rem(at_x + step, count_x)}

    def plane_target(step):
        spot = lax.rem(at_plane + step, count_plane)
        target = {"gy": lax.rem(spot // count_z, count_y), "gz": lax.rem(spot, count_z)}
        if direct:
            target["gx"] = spot // (count_y * count_z)
        return target

    barrier = pltpu.get_barrier_semaphore()
    for which in range(1, 8):
        pl.semaphore_signal(barrier, inc=1, device_id=neighbour(which, -1), device_id_type=MESH)
    for step in range(1, count_x):
        pl.semaphore_signal(barrier, inc=1, device_id=line_target(step), device_id_type=MESH)
    for step in range(1, count_plane):
        pl.semaphore_signal(barrier, inc=1, device_id=plane_target(step), device_id_type=MESH)
    pl.semaphore_wait(barrier, 7 + count_x - 1 + count_plane - 1)

    def send_plane():
        plane_copies = []
        for step in range(1, count_plane):
            copy = pltpu.make_async_remote_copy(
                src_ref=part if direct else middle,
                dst_ref=plane.at[at_plane],
                send_sem=plane_send.at[step],
                recv_sem=plane_recv.at[step],
                device_id=plane_target(step),
                device_id_type=MESH,
            )
            copy.start()
            plane_copies.append(copy)
        return plane_copies

    copies = []
    for which in range(1, 8):
        source = tuple(
            pl.ds(size, 1) if bit else pl.ds(0, size)
            for bit, size in zip(corner_of(which), sizes)
        )
        copy = pltpu.make_async_remote_copy(
            src_ref=reaction.at[source],
            dst_ref=landed[which - 1],
            send_sem=send_sem.at[which],
            recv_sem=recv_sem.at[which],
            device_id=neighbour(which, 1),
            device_id_type=MESH,
        )
        copy.start()
        copies.append(copy)
    line_copies = []
    for step in range(1, count_x):
        copy = pltpu.make_async_remote_copy(
            src_ref=part,
            dst_ref=line.at[at_x],
            send_sem=line_send.at[step],
            recv_sem=line_recv.at[step],
            device_id=line_target(step),
            device_id_type=MESH,
        )
        copy.start()
        line_copies.append(copy)
    if not direct:
        line[at_x] = part[...]
        for copy in line_copies:
            copy.wait()
        summed = line[0]
        for step in range(1, count_x):
            summed = summed + line[step]
        middle[...] = summed
        plane[at_plane] = summed
    else:
        plane_copies = send_plane()
        plane[at_plane] = part[...]
    for copy in copies:
        copy.wait()
    for x in range(sizes[0]):
        for y in range(sizes[1]):
            for z in range(sizes[2]):
                value = reaction[x, y, z]
                for which in range(1, 8):
                    bits = corner_of(which)
                    spot = (x, y, z)
                    if all(not bit or at == 0 for bit, at in zip(bits, spot)):
                        value = value + landed[which - 1][
                            tuple(0 if bit else at for bit, at in zip(bits, spot))
                        ]
                for axis in range(3):
                    forces[axis, x, y, pl.ds(z, 1)] = value[axis : axis + 1]
    if not direct:
        plane_copies = send_plane()
    for copy in plane_copies:
        copy.wait()
    summed = plane[0]
    for step in range(1, count_plane):
        summed = summed + plane[step]
    totals[0] = jnp.sum(summed[0:1]) * normaliser
    totals[1] = jnp.sum(summed[1:2]) * normaliser


def per_device(positions, type_ids, counts, type_charge, type_sigma, type_epsilon):
    types = type_charge.shape[0]
    sizes, width = type_ids.shape[:3], type_ids.shape[3]
    ext_sizes = tuple(size + 1 for size in sizes)
    cells = ext_sizes[0] * ext_sizes[1] * ext_sizes[2]
    vmem = pl.BlockSpec(memory_space=pltpu.VMEM)
    smem = pl.BlockSpec(memory_space=pltpu.SMEM)
    f32 = jnp.float32
    ext = pl.pallas_call(
        halo_kernel,
        name="halo",
        out_shape=jax.ShapeDtypeStruct(ext_sizes + (8, width), f32),
        in_specs=[vmem, vmem, smem],
        out_specs=vmem,
        scratch_shapes=[pltpu.VMEM(sizes + (8, width), f32), pltpu.SemaphoreType.DMA((8,)), pltpu.SemaphoreType.DMA((8,))],
        compiler_params=pltpu.CompilerParams(
            collective_id=0, has_side_effects=True, vmem_limit_bytes=8 * 1024 * 1024
        ),
    )(positions, type_ids, counts)
    pack = width // 4
    tiles = -(-cells // pack)
    reaction, part = pl.pallas_call(
        functools.partial(pair_kernel, types),
        name="pairs",
        out_shape=(
            jax.ShapeDtypeStruct(ext_sizes + (8, width), f32),
            jax.ShapeDtypeStruct((2, width), f32),
        ),
        in_specs=[smem, smem, smem, vmem],
        out_specs=(vmem, vmem),
        scratch_shapes=[
            pltpu.VMEM((tiles * width, width), f32),
            pltpu.VMEM((cells, 4, width // 8, 8, width), f32),
            pltpu.VMEM((cells, 3 + 5 * types, 8, width), f32),
            pltpu.VMEM(
                (len(second_of), sizes[0] * sizes[1] * sizes[2], 3, width // 8, 8, width), f32
            ),
            pltpu.VMEM((cells, 3, 8, width), f32),
            pltpu.SMEM((cells,), jnp.int32),
        ],
        compiler_params=pltpu.CompilerParams(vmem_limit_bytes=VMEM_LIMIT),
    )(type_charge, type_sigma, type_epsilon, ext)
    count_x, count_y, count_z = (lax.axis_size(axis) for axis in AXES)
    count_plane = count_y * count_z
    slots_x, slots_plane = count_x, count_plane
    if count_x * count_plane <= direct_limit:
        slots_x, slots_plane = 1, count_x * count_plane
    normaliser = 1.0 / (
        sizes[0] * count_x * sizes[1] * count_y * sizes[2] * count_z * width
    )
    landing = [
        pltpu.VMEM(
            tuple(1 if bit else size for bit, size in zip(corner_of(which), sizes)) + (8, width),
            f32,
        )
        for which in range(1, 8)
    ]
    forces, totals = pl.pallas_call(
        functools.partial(return_kernel, normaliser),
        name="giveback",
        out_shape=(
            jax.ShapeDtypeStruct((3,) + sizes + (width,), f32),
            jax.ShapeDtypeStruct((2,), f32),
        ),
        in_specs=[vmem, vmem],
        out_specs=(vmem, smem),
        scratch_shapes=landing
        + [
            pltpu.SemaphoreType.DMA((8,)),
            pltpu.SemaphoreType.DMA((8,)),
            pltpu.VMEM((slots_x, 2, width), f32),
            pltpu.VMEM((slots_plane, 2, width), f32),
            pltpu.VMEM((2, width), f32),
            pltpu.SemaphoreType.DMA((slots_x,)),
            pltpu.SemaphoreType.DMA((slots_x,)),
            pltpu.SemaphoreType.DMA((slots_plane,)),
            pltpu.SemaphoreType.DMA((slots_plane,)),
        ],
        compiler_params=pltpu.CompilerParams(
            collective_id=1, has_side_effects=True, vmem_limit_bytes=8 * 1024 * 1024
        ),
    )(reaction, part)
    return forces, totals


def solution(mesh):
    in_specs = (
        P(None, "gx", "gy", "gz", None),
        P("gx", "gy", "gz", None),
        P("gx", "gy", "gz"),
        P(),
        P(),
        P(),
    )
    out_specs = (P(None, "gx", "gy", "gz", None), P())
    return jax.shard_map(
        per_device, mesh=mesh, in_specs=in_specs, out_specs=out_specs, check_vma=False
    )
```
